256 devices in a mesh: region: 8 (over x, y_lo), scen: 32 (over y_hi, z, core).
Axes of the slice: x: 4, y: 4 (y_hi: 2, y_lo: 2; y = y_hi * 2 + y_lo), z: 8, core: 2. Of those that a mesh axis runs over, the one named last changes fastest.
Arguments:
- start_state: float32 [8, 512, 24, 1024], P('region', 'scen'), may hold values from -6 to 6
- price: float32 [8, 512, 24, 1024], P('region', 'scen'), may hold values from -6 to 6
- demand: float32 [8, 512, 24, 1024], P('region', 'scen'), may hold values from 0.2 to 2
- sens: bfloat16 [8, 1024, 1024], P('region'), as said below
- gen_bus: int32 [8, 512], P('region'), may hold values from 0 to 1023
- gen_cap: float32 [8, 512], P('region'), may hold values from 0.5 to 3
- tie_index: int32 [8, 2, 512], P('region'), may hold values from 0 to 1023, as said below
- tie_len: int32 [8, 2], P('region'), may hold values from 128 to 512, as said below
Outputs:
- final_state: float32 [8, 512, 24, 1024], P('region', 'scen')
- plan: float32 [8, 24, 1024], P('region')
The draws below stay inside these ranges and needn't reach their ends.
Inputs may be any that keep to these rules, and one draw needn't show every extreme that they name: `tie_index`: for each region the two rows together hold each of the 1024 bus numbers exactly once. tie_len[r, 1] equals tie_len[(r + 1) mod 8, 0]; some border has exactly 512 live slots. `sens`: each matrix has a positive diagonal between 0.5 and 2 and off-diagonal entries of order 1 / sqrt(1024).
All inputs are finite; a program needn't handle non-finite values.
Results may differ from the reference program's by a relative error of at most 0.00098.
Values sent between devices are 32-bit elements; how exact they have to be, the bound alone decides.
No kernel may reach another device: no remote copies, remote signals or barrier semaphores. Data moves between devices by JAX's collectives and lax.ppermute only.
A program may use at most 64 MiB of HBM per device.

```python
import math
import jax
import jax.numpy as jnp
from jax import lax

NB = 1024
TIE = 512
H = 24
G = 512
SWEEPS = 2
STEPS = 3
REGIONS = 8
SCEN = 512


def draw_sens(key, part):
    key_diag, key_off = jax.random.split(key, 2)
    diagonal = jnp.exp(jax.random.uniform(key_diag, (REGIONS, NB), jnp.float32, math.log(0.5), math.log(2.0)))
    off_part = jax.random.normal(key_off, (REGIONS, NB, NB), jnp.float32) * 0.5 / NB ** 0.5
    identity = jnp.eye(NB, dtype=jnp.float32)
    return (off_part * (1.0 - identity) + diagonal[:, :, None] * identity).astype(jnp.bfloat16)


def draw_tie_index(key, part):
    region_keys = jax.random.split(key, REGIONS)

    def one_region(region_key):
        return jax.random.permutation(region_key, NB).reshape(2, NB // 2)
    return jax.vmap(one_region)(region_keys).astype(jnp.int32)


def draw_tie_len(key, part):
    key_len, key_place = jax.random.split(key)
    border = jax.random.randint(key_len, (REGIONS,), TIE // 4, TIE + 1)
    chosen = jax.random.randint(key_place, (), 0, REGIONS)
    border = jnp.where(jnp.arange(REGIONS) == chosen, TIE, border)
    return jnp.stack([jnp.roll(border, 1), border], axis=1).astype(jnp.int32)


def set_ends(drawn, stream_key, low, top_value):
    longest = drawn.shape.index(max(drawn.shape))
    spots = []
    for shift in (0, 1):
        where = [jax.random.randint(jax.random.fold_in(stream_key, axis), (), 0, length) for axis, length in enumerate(drawn.shape)]
        where[longest] = (where[longest] + shift) % drawn.shape[longest]
        spots.append(tuple(where))
    return drawn.at[spots[0]].set(low).at[spots[1]].set(top_value)


def block_levels(key, extent, cuts, low, top_value):
    loudness = 1.0
    for position, parts in cuts:
        draws = jax.random.uniform(jax.random.fold_in(jax.random.fold_in(key, 6), position), (parts,), jnp.float32, low / len(cuts), top_value / len(cuts))
        loudness = loudness * jnp.repeat(jnp.exp(draws), extent[position] // parts).reshape((-1,) + (1,) * (len(extent) - 1 - position))
    return loudness


def normal_values(rng, extent, width, limit, pieces=(), kind=jnp.bfloat16):
    array = width * jax.random.normal(rng, extent, jnp.float32)
    if pieces:
        array = array * block_levels(rng, extent, pieces, -0.22, 0.18)
    return jnp.clip(array, -limit, limit).astype(kind)


def setup_inputs(seed: int = 0) -> dict:
    seeds = jax.random.split(jax.random.key(seed), 9)
    start_state = normal_values(seeds[0], (REGIONS, SCEN, H, NB), 1.0, 6.0, ((0, 8), (1, 32)), jnp.float32)
    price = normal_values(seeds[1], (REGIONS, SCEN, H, NB), 1.0, 6.0, ((0, 8), (1, 32)), jnp.float32)
    demand = jnp.clip(jnp.exp(math.log(2.0) - 2.3025851 * jax.random.uniform(seeds[2], (REGIONS, SCEN, H, NB), jnp.float32) ** block_levels(seeds[2], (REGIONS, SCEN, H, NB), ((0, 8), (1, 32)), -0.2, 0.2)), 0.2, 2.0)
    sens = draw_sens(jax.random.fold_in(seeds[8], 71), 0)
    gen_bus = set_ends(jax.random.randint(seeds[4], (REGIONS, G), 0, NB), jax.random.fold_in(seeds[4], 1), 0, NB - 1).astype(jnp.int32)
    gen_cap = jnp.clip(jnp.exp(math.log(3.0) - 1.7917595 * jax.random.uniform(seeds[5], (REGIONS, G), jnp.float32) ** block_levels(seeds[5], (REGIONS, G), ((0, 8),), -0.2, 0.2)), 0.5, 3.0)
    tie_index = draw_tie_index(jax.random.fold_in(seeds[8], 71), 0)
    tie_len = draw_tie_len(jax.random.fold_in(seeds[8], 71), 0)
    return {"start_state": start_state, "price": price, "demand": demand, "sens": sens, "gen_bus": gen_bus, "gen_cap": gen_cap, "tie_index": tie_index, "tie_len": tie_len}


step_rate = 0.3
tie_weight = 1.0
day_weight = 0.5


def pick_blocks(region_state, indices):
    return jnp.stack([region_state[..., indices[0]], region_state[..., indices[1]]])


def place_blocks(values, indices):
    placed = jnp.zeros(values.shape[1:3] + (NB,), jnp.float32)
    placed = placed.at[..., indices[0]].set(values[0])
    return placed.at[..., indices[1]].set(values[1])


def place_mask(live, indices):
    placed = jnp.zeros((NB,), jnp.float32)
    return placed.at[indices[0]].set(live[0]).at[indices[1]].set(live[1])


def add_caps(buses, capacity):
    return jnp.zeros((NB,), jnp.float32).at[buses].add(capacity)


def descend(items):
    state, price_part, demand_part, matrix, target, tie_mask, plan, day_dual, upper = items
    for repeat in range(STEPS):
        rounded = state.reshape(-1, NB).astype(jnp.bfloat16)
        slope = jnp.dot(rounded, matrix, preferred_element_type=jnp.float32).reshape(state.shape)
        slope = slope + price_part + tie_weight * tie_mask * (state - target) + day_weight * (state - plan + day_dual)
        state = jnp.clip(state - step_rate * slope, -demand_part, upper)
    return state


def reference(start_state, price, demand, sens, gen_bus, gen_cap, tie_index, tie_len):
    state = start_state
    live = (jnp.arange(TIE, dtype=jnp.int32)[None, None, :] < tie_len[:, :, None]).astype(jnp.float32)
    upper = jax.vmap(add_caps)(gen_bus, gen_cap)
    tie_mask = jax.vmap(place_mask)(live, tie_index)
    tie_dual = jnp.zeros((REGIONS, 2, SCEN, H, TIE), jnp.float32)
    day_dual = jnp.zeros_like(state)
    plan = jnp.zeros((REGIONS, H, NB), jnp.float32)
    for sweep in range(SWEEPS):
        blocks = jax.vmap(pick_blocks)(state, tie_index)
        from_left = jnp.roll(blocks[:, 1], 1, axis=0)
        from_right = jnp.roll(blocks[:, 0], -1, axis=0)
        theirs = jnp.stack([from_left, from_right], axis=1)
        middle = 0.5 * (blocks + theirs)
        tie_dual = tie_dual + blocks - middle
        target_blocks = (middle - tie_dual) * live[:, :, None, None, :]
        target = jax.vmap(place_blocks)(target_blocks, tie_index)
        plan = jnp.sum(state + day_dual, axis=1) / SCEN
        day_dual = day_dual + state - plan[:, None]
        state = lax.map(descend, (state, price, demand, sens, target, tie_mask, plan, day_dual, upper))
    return state, plan
```

```python
import jax
import jax.numpy as jnp
from jax import lax
from jax.experimental import pallas as pl
from jax.experimental.pallas import tpu as pltpu
from jax.sharding import PartitionSpec as P


CHUNKS = (6, 10)
BLOCK = 256
step_rate = 0.3
tie_weight = 1.0
day_weight = 0.5


F32 = jnp.float32
BF16 = jnp.bfloat16


def dot(a, b):
    return lax.dot_general(a, b, (((1,), (0,)), ((), ())), preferred_element_type=F32)


def dot_t(a, b):
    return lax.dot_general(a, b, (((1,), (1,)), ((), ())), preferred_element_type=F32)


def high_low(x):
    high = x.astype(BF16)
    return high, (x - high.astype(F32)).astype(BF16)


def call(kernel, outs, *, n_in, scratch=()):
    vmem = pl.BlockSpec(memory_space=pltpu.VMEM)
    return pl.pallas_call(
        kernel,
        out_shape=outs,
        in_specs=[vmem] * n_in,
        out_specs=jax.tree.map(lambda _: vmem, outs),
        scratch_shapes=list(scratch),
        compiler_params=pltpu.CompilerParams(vmem_limit_bytes=24 << 20),
    )


def over_scenarios(value, hours):
    rows, width = value.shape
    return jnp.sum(value.reshape(rows // hours, hours, width), axis=0)


def for_scenarios(value, rows):
    hours, width = value.shape
    return jnp.broadcast_to(value[None], (rows // hours, hours, width)).reshape(rows, width)


def sum_kernel(state, out):
    hours = out.shape[0]

    def one(n, _):
        at = pl.ds(pl.multiple_of(n * BLOCK, BLOCK), BLOCK)
        out[:, at] = over_scenarios(state[:, at], hours)
        return 0

    lax.fori_loop(0, out.shape[1] // BLOCK, one, 0)


def select_kernel(index, out):
    rows = 128

    def one(n, _):
        start = pl.multiple_of(n * rows, rows)
        bus = lax.broadcasted_iota(jnp.int32, (rows, out.shape[1]), 0) + start
        out[pl.ds(start, rows), :] = jnp.where(bus == index[...], 1.0, 0.0).astype(BF16)
        return 0

    lax.fori_loop(0, out.shape[0] // rows, one, 0)


def pick_into(pair, select, outs):
    rows, width = outs[0].shape

    for side, out in enumerate(outs):

        def one(n, _):
            at = pl.ds(pl.multiple_of(side * width + n * BLOCK, BLOCK), BLOCK)
            both = dot(pair[...], select[:, at])
            out[:, pl.ds(pl.multiple_of(n * BLOCK, BLOCK), BLOCK)] = both[:rows] + both[rows:]
            return 0

        lax.fori_loop(0, width // BLOCK, one, 0)


def split_into(pair, value, at):
    rows = value.shape[0]
    high, low = high_low(value)
    pair[:rows, at] = high
    pair[rows:, at] = low


def pick_kernel(start, state, select, *rest):
    outs, pair = rest[:2], rest[2]
    rows, _ = outs[0].shape

    def one(n, _):
        at = pl.ds(pl.multiple_of(n * BLOCK, BLOCK), BLOCK)
        split_into(pair, state[start : start + rows, at], at)
        return 0

    lax.fori_loop(0, state.shape[1] // BLOCK, one, 0)
    pick_into(pair, select, outs)


def bounds_kernel(select, live, gen_bus, gen_cap, mask, upper):
    mask[...] = dot_t(jnp.broadcast_to(live[...], (8, live.shape[1])).astype(BF16), select[...])
    caps = jnp.broadcast_to(gen_cap[...], (8, gen_cap.shape[1]))
    high, rest = high_low(caps)
    middle, low = high_low(caps - high.astype(F32))
    del rest
    three = jnp.concatenate([high, middle, low], axis=0)
    rows = 128

    def one(n, _):
        start = pl.multiple_of(n * rows, rows)
        bus = lax.broadcasted_iota(jnp.int32, (rows, gen_bus.shape[1]), 0) + start
        chosen = jnp.where(bus == gen_bus[...], 1.0, 0.0).astype(BF16)
        parts = dot_t(three, chosen)
        upper[:, pl.ds(start, rows)] = parts[:8] + parts[8:16] + parts[16:]
        return 0

    lax.fori_loop(0, upper.shape[1] // rows, one, 0)


def steps(state, rounded, base, matrix, demand, mask, upper, start, out, first, extra=None):
    rows, buses = state.shape
    blocks = buses // BLOCK

    def step(k, source, target_rounded, target, last):
        def one(n, _):
            at = pl.ds(pl.multiple_of(n * BLOCK, BLOCK), BLOCK)
            slope = dot(rounded[source], matrix[:, at])
            if k == 0:
                now = first(at)
            else:
                now = state[:, at]
            slope = slope + base[:, at] + (tie_weight * mask[:1, at] + day_weight) * now
            new = jnp.minimum(
                jnp.maximum(now - step_rate * slope, -demand[start : start + rows, at]), upper[:1, at]
            )
            target[:, at] = new
            if not last:
                rounded[target_rounded, :, at] = new.astype(BF16)
            elif extra is not None:
                extra(at, new)
            return 0

        lax.fori_loop(0, blocks, one, 0)

    step(0, 0, 1, state, False)
    step(1, 1, 0, state, False)
    step(2, 0, 1, out, True)


def first_kernel(start, state0, price, demand, matrix, select, left, right, mask, upper, plan, out, dual_out, total, picked_a, picked_b, state, rounded, base, pair):
    rows, buses = out.shape
    hours = plan.shape[0]
    slots = left.shape[1]

    def load(n, _):
        at = pl.ds(pl.multiple_of(n * BLOCK, BLOCK), BLOCK)
        rounded[0, :, at] = state0[start : start + rows, at].astype(BF16)
        return 0

    lax.fori_loop(0, buses // BLOCK, load, 0)
    split_into(pair, left[...], pl.ds(0, slots))
    split_into(pair, right[...], pl.ds(slots, slots))

    def first(at):
        return state0[start : start + rows, at]

    def constant(n, _):
        at = pl.ds(pl.multiple_of(n * BLOCK, BLOCK), BLOCK)
        both = dot_t(pair[...], select[at, :])
        theirs = both[:rows] + both[rows:]
        now = first(at)
        middle = 0.5 * (now + theirs)
        dual = now - middle
        target = mask[:1, at] * (middle - dual)
        dual_out[:, at] = dual
        day_plan = for_scenarios(plan[:, at], rows)
        day_dual = now - day_plan
        base[:, at] = (
            price[start : start + rows, at]
            - tie_weight * mask[:1, at] * target
            + day_weight * (day_dual - day_plan)
        )
        return 0

    lax.fori_loop(0, buses // BLOCK, constant, 0)

    def extra(at, new):
        split_into(pair, new, at)
        day_plan = for_scenarios(plan[:, at], rows)
        total[:, at] = over_scenarios(new + (first(at) - day_plan), hours)

    steps(state, rounded, base, matrix, demand, mask, upper, start, out, first, extra)
    pick_into(pair, select, (picked_a, picked_b))


def second_kernel(start, state0, state1, dual1, price, demand, matrix, select, left, right, mask, upper, plan1, plan2, out, state, rounded, base, pair):
    rows, buses = out.shape
    slots = left.shape[1]

    def load(n, _):
        at = pl.ds(pl.multiple_of(n * BLOCK, BLOCK), BLOCK)
        rounded[0, :, at] = state1[:, at].astype(BF16)
        return 0

    lax.fori_loop(0, buses // BLOCK, load, 0)
    split_into(pair, left[...], pl.ds(0, slots))
    split_into(pair, right[...], pl.ds(slots, slots))

    def first(at):
        return state1[:, at]

    def constant(n, _):
        at = pl.ds(pl.multiple_of(n * BLOCK, BLOCK), BLOCK)
        both = dot_t(pair[...], select[at, :])
        theirs = both[:rows] + both[rows:]
        now = first(at)
        middle = 0.5 * (now + theirs)
        dual = dual1[:, at] + now - middle
        target = mask[:1, at] * (middle - dual)
        day_plan = for_scenarios(plan2[:, at], rows)
        day_dual = state0[start : start + rows, at] - for_scenarios(plan1[:, at], rows)
        day_dual = day_dual + now - day_plan
        base[:, at] = (
            price[start : start + rows, at]
            - tie_weight * mask[:1, at] * target
            + day_weight * (day_dual - day_plan)
        )
        return 0

    lax.fori_loop(0, buses // BLOCK, constant, 0)
    steps(state, rounded, base, matrix, demand, mask, upper, start, out, first)


def flipped(size, bit):
    return [(i, i ^ bit) for i in range(size)]


def borders(size, first):
    pairs = [((i + first) % size, (i + first + 1) % size) for i in range(0, size, 2)]
    return [pair for a, b in pairs for pair in ((a, b), (b, a))]


def exchange(a, b):
    size = lax.axis_size("region")
    return (
        lax.ppermute(a, "region", borders(size, 0)),
        lax.ppermute(b, "region", borders(size, 1)),
    )


def summed(total, core):
    size = lax.axis_size("scen")
    half = total.shape[1] // 2
    mine = jnp.where(core == 0, total[:, :half], total[:, half:])
    other = jnp.where(core == 0, total[:, half:], total[:, :half])
    part = mine + lax.ppermute(other, "scen", flipped(size, 1))
    for group in ((size // 2,), (2,), (4, 8, 12)):
        others = []
        for bit in group:
            others.append(lax.ppermute(part, "scen", flipped(size, bit)))
        part = part + others[0]
        if len(group) > 1:
            part = part + (others[1] + others[2])
    back = lax.ppermute(part, "scen", flipped(size, 1))
    return jnp.where(
        core == 0, jnp.concatenate([part, back], axis=1), jnp.concatenate([back, part], axis=1)
    )


def inner(start_state, price, demand, sens, gen_bus, gen_cap, tie_index, tie_len):
    scens, hours, buses = start_state.shape[1:]
    slots = tie_index.shape[2]
    rows = scens * hours
    total_scen = scens * lax.axis_size("scen")
    state0 = start_state.reshape(rows, buses)
    prices = price.reshape(rows, buses)
    demands = demand.reshape(rows, buses)
    matrix = sens[0]
    core = lax.axis_index("scen") % 2
    odd = lax.axis_index("region") % 2

    def by_border(pair):
        return jnp.where(odd == 0, jnp.concatenate([pair[1], pair[0]]), jnp.concatenate([pair[0], pair[1]]))[None]

    index = by_border(tie_index[0])
    live = (jnp.arange(slots, dtype=jnp.int32)[None, :] < tie_len[0][:, None]).astype(F32)
    live = by_border(live)

    def shape(*dims, dtype=F32):
        return jax.ShapeDtypeStruct(dims, dtype)

    total0 = call(sum_kernel, shape(hours, buses), n_in=1)(state0)
    select = call(select_kernel, shape(buses, 2 * slots, dtype=BF16), n_in=1)(index)
    starts = [sum(CHUNKS[:c]) * hours for c in range(len(CHUNKS))]
    sizes = [c * hours for c in CHUNKS]
    theirs = []
    for at, size in zip(starts, sizes):
        picked = call(
            lambda *refs, at=at: pick_kernel(at, *refs),
            (shape(size, slots), shape(size, slots)),
            n_in=2,
            scratch=[pltpu.VMEM((2 * size, buses), BF16)],
        )(state0, select)
        theirs.append(exchange(*picked))
    mask, upper = call(bounds_kernel, (shape(8, buses), shape(8, buses)), n_in=4)(
        select, live, gen_bus, gen_cap
    )
    plan1 = summed(total0, core) / total_scen

    def scratch(size):
        return [
            pltpu.VMEM((size, buses), F32),
            pltpu.VMEM((2, size, buses), BF16),
            pltpu.VMEM((size, buses), F32),
            pltpu.VMEM((2 * size, buses), BF16),
        ]

    firsts = []
    theirs1 = []
    for c, (at, size) in enumerate(zip(starts, sizes)):
        first = call(
            lambda *refs, at=at: first_kernel(at, *refs),
            (
                shape(size, buses),
                shape(size, buses),
                shape(hours, buses),
                shape(size, slots),
                shape(size, slots),
            ),
            n_in=10,
            scratch=scratch(size),
        )(state0, prices, demands, matrix, select, *theirs[c], mask, upper, plan1)
        firsts.append(first)
        theirs1.append(exchange(first[3], first[4]))
    total1 = sum(f[2] for f in firsts[1:]) + firsts[0][2]
    plan2 = summed(total1, core) / total_scen
    finals = []
    for c, (at, size) in enumerate(zip(starts, sizes)):
        final = call(
            lambda *refs, at=at: second_kernel(at, *refs),
            shape(size, buses),
            n_in=13,
            scratch=scratch(size),
        )(state0, firsts[c][0], firsts[c][1], prices, demands, matrix, select, *theirs1[c], mask, upper, plan1, plan2)
        finals.append(final)
    final_state = jnp.concatenate(finals, axis=0).reshape(scens, hours, buses)
    return (final_state[None], plan2[None])


def solution(mesh):
    in_specs = (
        P("region", "scen", None, None),
        P("region", "scen", None, None),
        P("region", "scen", None, None),
        P("region", None, None),
        P("region", None),
        P("region", None),
        P("region", None, None),
        P("region", None),
    )
    out_specs = (P("region", "scen", None, None), P("region", None, None))
    return jax.shard_map(inner, mesh=mesh, in_specs=in_specs, out_specs=out_specs, check_vma=False)
```

```python
import jax
import jax.numpy as jnp
from jax import lax
from jax.experimental import pallas as pl
from jax.experimental.pallas import tpu as pltpu
from jax.sharding import PartitionSpec as P


CHUNKS = (6, 10)
BLOCK = 256
step_rate = 0.3
tie_weight = 1.0
day_weight = 0.5


F32 = jnp.float32
BF16 = jnp.bfloat16


def dot(a, b):
    return lax.dot_general(a, b, (((1,), (0,)), ((), ())), preferred_element_type=F32)


def dot_t(a, b):
    return lax.dot_general(a, b, (((1,), (1,)), ((), ())), preferred_element_type=F32)


def high_low(x):
    high = x.astype(BF16)
    return high, (x - high.astype(F32)).astype(BF16)


def call(kernel, outs, *, n_in, scratch=()):
    vmem = pl.BlockSpec(memory_space=pltpu.VMEM)
    return pl.pallas_call(
        kernel,
        out_shape=outs,
        in_specs=[vmem] * n_in,
        out_specs=jax.tree.map(lambda _: vmem, outs),
        scratch_shapes=list(scratch),
        compiler_params=pltpu.CompilerParams(vmem_limit_bytes=24 << 20),
    )


def over_scenarios(value, hours):
    rows, width = value.shape
    return jnp.sum(value.reshape(rows // hours, hours, width), axis=0)


def for_scenarios(value, rows):
    hours, width = value.shape
    return jnp.broadcast_to(value[None], (rows // hours, hours, width)).reshape(rows, width)


def over_blocks(width, one):
    for n in range(width // BLOCK):
        one(pl.ds(n * BLOCK, BLOCK))


def sum_kernel(state, out):
    hours = out.shape[0]

    def one(n, _):
        at = pl.ds(pl.multiple_of(n * BLOCK, BLOCK), BLOCK)
        out[:, at] = over_scenarios(state[:, at], hours)
        return 0

    lax.fori_loop(0, out.shape[1] // BLOCK, one, 0)


def select_kernel(index, out):
    rows = 128

    def one(n, _):
        start = pl.multiple_of(n * rows, rows)
        bus = lax.broadcasted_iota(jnp.int32, (rows, out.shape[1]), 0) + start
        out[pl.ds(start, rows), :] = jnp.where(bus == index[...], 1.0, 0.0).astype(BF16)
        return 0

    lax.fori_loop(0, out.shape[0] // rows, one, 0)


def split_into(pair, value, at):
    rows = value.shape[0]
    high, low = high_low(value)
    pair[:rows, at] = high
    pair[rows:, at] = low


def pick_kernel(start, state, select, left, right, pair):
    rows, slots = left.shape
    over_blocks(state.shape[1], lambda at: split_into(pair, state[start : start + rows, at], at))

    def one(at):
        both = dot(pair[...], select[:, at])
        out, base = (left, 0) if at.start < slots else (right, slots)
        out[:, pl.ds(at.start - base, at.size)] = both[:rows] + both[rows:]

    over_blocks(2 * slots, one)


def bounds_kernel(select, live, gen_bus, gen_cap, mask, upper):
    mask[...] = dot_t(jnp.broadcast_to(live[...], (8, live.shape[1])).astype(BF16), select[...])
    caps = jnp.broadcast_to(gen_cap[...], (8, gen_cap.shape[1]))
    high, rest = high_low(caps)
    middle, low = high_low(caps - high.astype(F32))
    del rest
    three = jnp.concatenate([high, middle, low], axis=0)
    rows = 128

    def one(n, _):
        start = pl.multiple_of(n * rows, rows)
        bus = lax.broadcasted_iota(jnp.int32, (rows, gen_bus.shape[1]), 0) + start
        chosen = jnp.where(bus == gen_bus[...], 1.0, 0.0).astype(BF16)
        parts = dot_t(three, chosen)
        upper[:, pl.ds(start, rows)] = parts[:8] + parts[8:16] + parts[16:]
        return 0

    lax.fori_loop(0, upper.shape[1] // rows, one, 0)


def theirs_into(pair, left, right):
    slots = left.shape[1]
    split_into(pair, left[...], pl.ds(0, slots))
    split_into(pair, right[...], pl.ds(slots, slots))


def theirs_at(pair, select, at):
    both = dot_t(pair[...], select[at, :])
    rows = both.shape[0] // 2
    return both[:rows] + both[rows:]


def stepped(now, slope, base, mask, lower, upper):
    slope = slope + base + (tie_weight * mask + day_weight) * now
    return jnp.minimum(jnp.maximum(now - step_rate * slope, lower), upper)


def first_kernel(start, state0, price, demand, matrix, select, left, right, mask, upper, plan, out, dual_out, total, even, other, base, pair):
    rows, buses = out.shape
    hours = plan.shape[0]
    part = slice(start, start + rows)
    theirs_into(pair, left, right)

    def load(at):
        even[:, at] = state0[part, at].astype(BF16)

    over_blocks(buses, load)

    def zero(at):
        now = state0[part, at]
        theirs = theirs_at(pair, select, at)
        middle = 0.5 * (now + theirs)
        dual = now - middle
        target = mask[:1, at] * (middle - dual)
        dual_out[:, at] = dual
        day_plan = for_scenarios(plan[:, at], rows)
        day_dual = now - day_plan
        constant = price[part, at] - tie_weight * mask[:1, at] * target + day_weight * (day_dual - day_plan)
        base[:, at] = constant
        new = stepped(now, dot(even[...], matrix[:, at]), constant, mask[:1, at], -demand[part, at], upper[:1, at])
        out[:, at] = new
        other[:, at] = new.astype(BF16)

    def one(at):
        new = stepped(out[:, at], dot(other[...], matrix[:, at]), base[:, at], mask[:1, at], -demand[part, at], upper[:1, at])
        out[:, at] = new
        even[:, at] = new.astype(BF16)

    def two(at):
        new = stepped(out[:, at], dot(even[...], matrix[:, at]), base[:, at], mask[:1, at], -demand[part, at], upper[:1, at])
        out[:, at] = new
        day_plan = for_scenarios(plan[:, at], rows)
        total[:, at] = over_scenarios(new + (state0[part, at] - day_plan), hours)

    over_blocks(buses, zero)
    over_blocks(buses, one)
    over_blocks(buses, two)


def prepare_kernel(start, state0, state1, dual1, price, select, left, right, mask, plan1, base, pair):
    rows, buses = base.shape
    part = slice(start, start + rows)
    theirs_into(pair, left, right)

    def zero(at):
        now = state1[:, at]
        middle = 0.5 * (now + theirs_at(pair, select, at))
        dual = dual1[:, at] + now - middle
        target = mask[:1, at] * (middle - dual)
        day_dual = state0[part, at] - for_scenarios(plan1[:, at], rows)
        base[:, at] = price[part, at] - tie_weight * mask[:1, at] * target + day_weight * (day_dual + now)

    over_blocks(buses, zero)


def final_kernel(*refs):
    count = len(CHUNKS)
    states, bases = refs[:count], refs[count : 2 * count]
    demand, matrix, mask, upper, plan, out, plan_out, even, other, base = refs[2 * count :]
    buses = out.shape[1]
    ends = [sum(r.shape[0] for r in states[:c]) for c in range(count + 1)]
    plan_out[...] = plan[...]

    def load(at):
        for c in range(count):
            even[ends[c] : ends[c + 1], at] = states[c][:, at].astype(BF16)

    over_blocks(buses, load)

    def step(source, target, first, last):
        def one(at):
            slope = dot(source[...], matrix[:, at])
            for c in range(count):
                part = slice(ends[c], ends[c + 1])
                if first:
                    day_plan = for_scenarios(plan[:, at], ends[c + 1] - ends[c])
                    constant = bases[c][:, at] - 2 * day_weight * day_plan
                    base[part, at] = constant
                    now = states[c][:, at]
                else:
                    constant = base[part, at]
                    now = out[part, at]
                new = stepped(now, slope[part], constant, mask[:1, at], -demand[part, at], upper[:1, at])
                out[part, at] = new
                if not last:
                    target[part, at] = new.astype(BF16)

        over_blocks(buses, one)

    step(even, other, True, False)
    step(other, even, False, False)
    step(even, other, False, True)


def flipped(size, bit):
    return [(i, i ^ bit) for i in range(size)]


def borders(size, first):
    pairs = [((i + first) % size, (i + first + 1) % size) for i in range(0, size, 2)]
    return [pair for a, b in pairs for pair in ((a, b), (b, a))]


def exchange(a, b):
    size = lax.axis_size("region")
    return (
        lax.ppermute(a, "region", borders(size, 0)),
        lax.ppermute(b, "region", borders(size, 1)),
    )


def summed(total, core):
    size = lax.axis_size("scen")
    half = total.shape[1] // 2
    mine = jnp.where(core == 0, total[:, :half], total[:, half:])
    other = jnp.where(core == 0, total[:, half:], total[:, :half])
    part = mine + lax.ppermute(other, "scen", flipped(size, 1))
    for group in ((size // 2,), (2,), (4, 8, 12)):
        others = []
        for bit in group:
            others.append(lax.ppermute(part, "scen", flipped(size, bit)))
        part = part + others[0]
        if len(group) > 1:
            part = part + (others[1] + others[2])
    back = lax.ppermute(part, "scen", flipped(size, 1))
    return jnp.where(
        core == 0, jnp.concatenate([part, back], axis=1), jnp.concatenate([back, part], axis=1)
    )


def inner(start_state, price, demand, sens, gen_bus, gen_cap, tie_index, tie_len):
    scens, hours, buses = start_state.shape[1:]
    slots = tie_index.shape[2]
    rows = scens * hours
    total_scen = scens * lax.axis_size("scen")
    state0 = start_state.reshape(rows, buses)
    prices = price.reshape(rows, buses)
    demands = demand.reshape(rows, buses)
    matrix = sens[0]
    core = lax.axis_index("scen") % 2
    odd = lax.axis_index("region") % 2

    def by_border(pair):
        return jnp.where(odd == 0, jnp.concatenate([pair[1], pair[0]]), jnp.concatenate([pair[0], pair[1]]))[None]

    index = by_border(tie_index[0])
    live = (jnp.arange(slots, dtype=jnp.int32)[None, :] < tie_len[0][:, None]).astype(F32)
    live = by_border(live)

    def shape(*dims, dtype=F32):
        return jax.ShapeDtypeStruct(dims, dtype)

    def pick(at, state, size):
        return call(
            lambda *refs: pick_kernel(at, *refs),
            (shape(size, slots), shape(size, slots)),
            n_in=2,
            scratch=[pltpu.VMEM((2 * size, buses), BF16)],
        )(state, select)

    total0 = call(sum_kernel, shape(hours, buses), n_in=1)(state0)
    select = call(select_kernel, shape(buses, 2 * slots, dtype=BF16), n_in=1)(index)
    starts = [sum(CHUNKS[:c]) * hours for c in range(len(CHUNKS))]
    sizes = [c * hours for c in CHUNKS]
    theirs = []
    for at, size in zip(starts, sizes):
        picked = pick(at, state0, size)
        theirs.append(exchange(*picked))
    mask, upper = call(bounds_kernel, (shape(8, buses), shape(8, buses)), n_in=4)(select, live, gen_bus, gen_cap)
    plan1 = summed(total0, core) / total_scen

    firsts = []
    theirs1 = []
    for c, (at, size) in enumerate(zip(starts, sizes)):
        wide = shape(size, buses)
        first = call(
            lambda *refs, at=at: first_kernel(at, *refs),
            (wide, wide, shape(hours, buses)),
            n_in=10,
            scratch=[
                pltpu.VMEM((size, buses), BF16),
                pltpu.VMEM((size, buses), BF16),
                pltpu.VMEM((size, buses), F32),
                pltpu.VMEM((2 * size, buses), BF16),
            ],
        )(state0, prices, demands, matrix, select, *theirs[c], mask, upper, plan1)
        firsts.append(first)
        picked = pick(0, first[0], size)
        theirs1.append(exchange(*picked))
    total1 = sum(f[2] for f in firsts[1:]) + firsts[0][2]
    bases = []
    for c, (at, size) in enumerate(zip(starts, sizes)):
        bases.append(
            call(
                lambda *refs, at=at: prepare_kernel(at, *refs),
                shape(size, buses),
                n_in=9,
                scratch=[pltpu.VMEM((2 * size, buses), BF16)],
            )(state0, firsts[c][0], firsts[c][1], prices, select, *theirs1[c], mask, plan1)
        )
    plan2 = summed(total1, core) / total_scen
    final_state, plan2 = call(
        final_kernel,
        (shape(rows, buses), shape(hours, buses)),
        n_in=2 * len(CHUNKS) + 5,
        scratch=[
            pltpu.VMEM((rows, buses), BF16),
            pltpu.VMEM((rows, buses), BF16),
            pltpu.VMEM((rows, buses), F32),
        ],
    )(*[f[0] for f in firsts], *bases, demands, matrix, mask, upper, plan2)
    return (final_state.reshape(start_state.shape), plan2[None])


def solution(mesh):
    in_specs = (
        P("region", "scen", None, None),
        P("region", "scen", None, None),
        P("region", "scen", None, None),
        P("region", None, None),
        P("region", None),
        P("region", None),
        P("region", None, None),
        P("region", None),
    )
    out_specs = (P("region", "scen", None, None), P("region", None, None))
    return jax.shard_map(inner, mesh=mesh, in_specs=in_specs, out_specs=out_specs, check_vma=False)
```

```python
import jax
import jax.numpy as jnp
from jax import lax
from jax.experimental import pallas as pl
from jax.experimental.pallas import tpu as pltpu
from jax.sharding import PartitionSpec as P


CHUNKS = (10, 6)
PARTS = ((4, 2, 4), (6,))
BLOCK = 256
step_rate = 0.3
tie_weight = 1.0
day_weight = 0.5


F32 = jnp.float32
BF16 = jnp.bfloat16


def dot(a, b):
    return lax.dot_general(a, b, (((1,), (0,)), ((), ())), preferred_element_type=F32)


def dot_t(a, b):
    return lax.dot_general(a, b, (((1,), (1,)), ((), ())), preferred_element_type=F32)


def high_low(x):
    high = x.astype(BF16)
    return high, (x - high.astype(F32)).astype(BF16)


def call(kernel, outs, *, n_in, scratch=(), out_space=pltpu.VMEM, flops=4 << 30):
    vmem = pl.BlockSpec(memory_space=pltpu.VMEM)
    out_spec = pl.BlockSpec(memory_space=out_space)
    return pl.pallas_call(
        kernel,
        out_shape=outs,
        in_specs=[vmem] * n_in,
        out_specs=jax.tree.map(lambda _: out_spec, outs),
        scratch_shapes=list(scratch),
        compiler_params=pltpu.CompilerParams(vmem_limit_bytes=16 << 20),
        cost_estimate=pl.CostEstimate(flops=flops, transcendentals=0, bytes_accessed=1 << 20),
    )


def over_scenarios(value, hours):
    rows, width = value.shape
    return jnp.sum(value.reshape(rows // hours, hours, width), axis=0)


def for_scenarios(value, rows):
    hours, width = value.shape
    return jnp.broadcast_to(value[None], (rows // hours, hours, width)).reshape(rows, width)


def over_blocks(width, one):
    for n in range(width // BLOCK):
        one(pl.ds(n * BLOCK, BLOCK))


def sum_kernel(state, out):
    hours = out.shape[0]

    def one(n, _):
        at = pl.ds(pl.multiple_of(n * BLOCK, BLOCK), BLOCK)
        out[:, at] = over_scenarios(state[:, at], hours)
        return 0

    lax.fori_loop(0, out.shape[1] // BLOCK, one, 0)


def select_kernel(index, out):
    rows = 128

    def one(n, _):
        start = pl.multiple_of(n * rows, rows)
        bus = lax.broadcasted_iota(jnp.int32, (rows, out.shape[1]), 0) + start
        out[pl.ds(start, rows), :] = jnp.where(bus == index[...], 1.0, 0.0).astype(BF16)
        return 0

    lax.fori_loop(0, out.shape[0] // rows, one, 0)


def split_into(pair, value, at):
    rows = value.shape[0]
    high, low = high_low(value)
    pair[:rows, at] = high
    pair[rows:, at] = low


def pick_kernel(start, state, select, left, right, pair):
    rows, slots = left.shape
    over_blocks(state.shape[1], lambda at: split_into(pair, state[start : start + rows, at], at))

    def one(at):
        both = dot(pair[...], select[:, at])
        out, base = (left, 0) if at.start < slots else (right, slots)
        out[:, pl.ds(at.start - base, at.size)] = both[:rows] + both[rows:]

    over_blocks(2 * slots, one)


def bounds_kernel(select, live, gen_bus, gen_cap, mask, upper):
    mask[...] = dot_t(jnp.broadcast_to(live[...], (8, live.shape[1])).astype(BF16), select[...])
    caps = jnp.broadcast_to(gen_cap[...], (8, gen_cap.shape[1]))
    high, rest = high_low(caps)
    middle, low = high_low(caps - high.astype(F32))
    del rest
    three = jnp.concatenate([high, middle, low], axis=0)
    rows = 128

    def one(n, _):
        start = pl.multiple_of(n * rows, rows)
        bus = lax.broadcasted_iota(jnp.int32, (rows, gen_bus.shape[1]), 0) + start
        chosen = jnp.where(bus == gen_bus[...], 1.0, 0.0).astype(BF16)
        parts = dot_t(three, chosen)
        upper[:, pl.ds(start, rows)] = parts[:8] + parts[8:16] + parts[16:]
        return 0

    lax.fori_loop(0, upper.shape[1] // rows, one, 0)


def theirs_into(pair, *ties):
    rows, at = pair.shape[0] // 2, 0
    for left, right in zip(ties[::2], ties[1::2]):
        size, slots = left.shape
        for start, side in ((0, left), (slots, right)):
            high, low = high_low(side[...])
            pair[at : at + size, start : start + slots] = high
            pair[rows + at : rows + at + size, start : start + slots] = low
        at += size


def theirs_at(pair, select, at):
    both = dot_t(pair[...], select[at, :])
    rows = both.shape[0] // 2
    return both[:rows] + both[rows:]


def stepped(now, slope, base, mask, lower, upper):
    slope = slope + base + (tie_weight * mask + day_weight) * now
    return jnp.minimum(jnp.maximum(now - step_rate * slope, lower), upper)


def first_kernel(start, *refs):
    state0, slope0, price, demand, matrix, select, left, right, mask, upper, plan = refs[:11]
    refs = refs[11:]
    out, dual_out, total, even, other, base, pair = refs
    rows, buses = out.shape
    hours = plan.shape[0]
    part = slice(start, start + rows)
    theirs_into(pair, left, right)

    def zero(at):
        now = state0[part, at]
        theirs = theirs_at(pair, select, at)
        middle = 0.5 * (now + theirs)
        dual = now - middle
        target = mask[:1, at] * (middle - dual)
        dual_out[:, at] = dual
        day_plan = for_scenarios(plan[:, at], rows)
        day_dual = now - day_plan
        constant = price[part, at] - tie_weight * mask[:1, at] * target + day_weight * (day_dual - day_plan)
        base[:, at] = constant
        new = stepped(now, slope0[part, at], constant, mask[:1, at], -demand[part, at], upper[:1, at])
        out[:, at] = new
        other[:, at] = new.astype(BF16)

    def one(at):
        new = stepped(out[:, at], dot(other[...], matrix[:, at]), base[:, at], mask[:1, at], -demand[part, at], upper[:1, at])
        out[:, at] = new
        even[:, at] = new.astype(BF16)

    def two(at):
        new = stepped(out[:, at], dot(even[...], matrix[:, at]), base[:, at], mask[:1, at], -demand[part, at], upper[:1, at])
        out[:, at] = new
        day_plan = for_scenarios(plan[:, at], rows)
        total[:, at] = over_scenarios(new + (state0[part, at] - day_plan), hours)

    over_blocks(buses, zero)
    over_blocks(buses, one)
    over_blocks(buses, two)


def prepare_kernel(start, inside, state0, state1, dual1, price, select, left, right, mask, plan1, base, pair):
    rows, buses = base.shape
    part = slice(start, start + rows)
    inner = slice(inside, inside + rows)
    theirs_into(pair, left, right)

    def zero(at):
        now = state1[inner, at]
        middle = 0.5 * (now + theirs_at(pair, select, at))
        dual = dual1[inner, at] + now - middle
        target = mask[:1, at] * (middle - dual)
        day_dual = state0[part, at] - for_scenarios(plan1[:, at], rows)
        base[:, at] = price[part, at] - tie_weight * mask[:1, at] * target + day_weight * (day_dual + now)

    over_blocks(buses, zero)


def early_kernel(state, matrix, slope, rounded):
    over_blocks(state.shape[1], lambda at: rounded.__setitem__((slice(None), at), state[:, at].astype(BF16)))

    def one(at):
        slope[:, at] = dot(rounded[...], matrix[:, at])

    over_blocks(state.shape[1], one)


def last_steps(start, insides, refs, written=None):
    pieces = [refs[3 * k : 3 * k + 3] for k in range(len(insides))]
    demand, matrix, mask, upper, plan, out, even, other, constants = refs[3 * len(insides) :]
    rows, buses = out.shape
    part = slice(start, start + rows)

    def zero(at):
        top = 0
        for inside, (state, slope, base) in zip(insides, pieces):
            size = base.shape[0]
            inner, here = slice(inside, inside + size), slice(top, top + size)
            lower = -demand[start + top : start + top + size, at]
            constant = base[:, at] - 2 * day_weight * for_scenarios(plan[:, at], size)
            constants[here, at] = constant
            new = stepped(state[inner, at], slope[inner, at], constant, mask[:1, at], lower, upper[:1, at])
            out[here, at] = new
            even[here, at] = new.astype(BF16)
            top += size

    def one(at):
        new = stepped(out[:, at], dot(even[...], matrix[:, at]), constants[:, at], mask[:1, at], -demand[part, at], upper[:1, at])
        out[:, at] = new
        other[:, at] = new.astype(BF16)

    def two(at):
        new = stepped(out[:, at], dot(other[...], matrix[:, at]), constants[:, at], mask[:1, at], -demand[part, at], upper[:1, at])
        out[:, at] = new
        if written is not None:
            written(at)

    over_blocks(buses, zero)
    over_blocks(buses, one)
    over_blocks(buses, two)


def middle_kernel(start, insides, *refs):
    last_steps(start, insides, refs)


def end_kernel(start, insides, done, *refs):
    ins = refs[: 3 * len(insides) + 5]
    whole, plan_out, out, even, other, constants, sems = refs[3 * len(insides) + 5 :]
    rows, _ = out.shape
    copies = [
        pltpu.make_async_copy(ins[-1], plan_out, sems.at[0]),
        pltpu.make_async_copy(done, whole.at[pl.ds(0, done.shape[0]), :], sems.at[1]),
    ]
    for copy in copies:
        copy.start()

    def written(at):
        copy = pltpu.make_async_copy(
            out.at[:, at], whole.at[pl.ds(start, rows), at], sems.at[2 + at.start // BLOCK]
        )
        copy.start()
        copies.append(copy)

    last_steps(start, insides, (*ins, out, even, other, constants), written)
    for copy in copies:
        copy.wait()


def flipped(size, bit):
    return [(i, i ^ bit) for i in range(size)]


def borders(size, first):
    pairs = [((i + first) % size, (i + first + 1) % size) for i in range(0, size, 2)]
    return [pair for a, b in pairs for pair in ((a, b), (b, a))]


def exchange(a, b):
    size = lax.axis_size("region")
    return (
        lax.ppermute(a, "region", borders(size, 0)),
        lax.ppermute(b, "region", borders(size, 1)),
    )


def halves(total, core):
    size = lax.axis_size("scen")
    half = total.shape[1] // 2
    mine = jnp.where(core == 0, total[:, :half], total[:, half:])
    other = jnp.where(core == 0, total[:, half:], total[:, :half])
    return mine + lax.ppermute(other, "scen", flipped(size, 1))


def joined(part, core):
    back = lax.ppermute(part, "scen", flipped(lax.axis_size("scen"), 1))
    return jnp.where(
        core == 0, jnp.concatenate([part, back], axis=1), jnp.concatenate([back, part], axis=1)
    )


def from_flipped(value, bit):
    return lax.ppermute(value, "scen", flipped(lax.axis_size("scen"), bit))


def summed(total, core):
    part = halves(total, core)
    for bit in (16, 2):
        part = part + from_flipped(part, bit)
    a, b, c = [from_flipped(part, bit) for bit in (4, 8, 12)]
    return joined((part + a) + (b + c), core)


def inner(start_state, price, demand, sens, gen_bus, gen_cap, tie_index, tie_len):
    scens, hours, buses = start_state.shape[1:]
    slots = tie_index.shape[2]
    rows = scens * hours
    total_scen = scens * lax.axis_size("scen")
    state0 = start_state.reshape(rows, buses)
    prices = price.reshape(rows, buses)
    demands = demand.reshape(rows, buses)
    matrix = sens[0]
    core = lax.axis_index("scen") % 2
    odd = lax.axis_index("region") % 2

    def by_border(pair):
        return jnp.where(odd == 0, jnp.concatenate([pair[1], pair[0]]), jnp.concatenate([pair[0], pair[1]]))[None]

    index = by_border(tie_index[0])
    live = (jnp.arange(slots, dtype=jnp.int32)[None, :] < tie_len[0][:, None]).astype(F32)
    live = by_border(live)

    def shape(*dims, dtype=F32):
        return jax.ShapeDtypeStruct(dims, dtype)

    def pick(at, state, size):
        return call(
            lambda *refs: pick_kernel(at, *refs),
            (shape(size, slots), shape(size, slots)),
            n_in=2,
            scratch=[pltpu.VMEM((2 * size, buses), BF16)],
        )(state, select)

    total0 = call(sum_kernel, shape(hours, buses), n_in=1, flops=1 << 20)(state0)
    select = call(select_kernel, shape(buses, 2 * slots, dtype=BF16), n_in=1, flops=1 << 20)(index)
    starts = [sum(CHUNKS[:c]) * hours for c in range(len(CHUNKS))]
    sizes = [c * hours for c in CHUNKS]
    theirs = []
    for at, size in zip(starts, sizes):
        picked = pick(at, state0, size)
        theirs.append(exchange(*picked))

    def early(state):
        return call(early_kernel, shape(*state.shape), n_in=2, scratch=[pltpu.VMEM(state.shape, BF16)])(state, matrix)

    slope0 = early(state0)
    mask, upper = call(bounds_kernel, (shape(8, buses), shape(8, buses)), n_in=4)(select, live, gen_bus, gen_cap)
    plan1 = summed(total0, core) / total_scen

    firsts = []
    theirs1 = []
    for c, (at, size) in enumerate(zip(starts, sizes)):
        wide = shape(size, buses)
        first = call(
            lambda *refs, at=at: first_kernel(at, *refs),
            (wide, wide, shape(hours, buses)),
            n_in=11,
            scratch=[
                pltpu.VMEM((size, buses), BF16),
                pltpu.VMEM((size, buses), BF16),
                pltpu.VMEM((size, buses), F32),
                pltpu.VMEM((2 * size, buses), BF16),
            ],
        )(state0, slope0, prices, demands, matrix, select, *theirs[c], mask, upper, plan1)
        firsts.append(first)
        inside = 0
        for k, part in enumerate(PARTS[c]):
            picked = pick(inside, first[0], part * hours)
            theirs1.append((c, k, inside, part * hours, exchange(*picked)))
            inside += part * hours
    total1 = sum(f[2] for f in firsts[1:]) + firsts[0][2]
    slopes = [early(first[0]) for first in firsts]
    pieces = []
    for c, k, inside, size, ties in theirs1:
        base = call(
            lambda *refs, at=starts[c] + inside, inside=inside: prepare_kernel(at, inside, *refs),
            shape(size, buses),
            n_in=9,
            scratch=[pltpu.VMEM((2 * size, buses), BF16)],
        )(state0, firsts[c][0], firsts[c][1], prices, select, *ties, mask, plan1)
        pieces.append((inside, size, (firsts[c][0], slopes[c], base)))
    plan2 = summed(total1, core) / total_scen
    common = (demands, matrix, mask, upper, plan2)

    def ending(kernel, at, parts, before, outs, **more):
        size = sum(p[1] for p in parts)
        insides = tuple(p[0] for p in parts)
        ins = (*before, *[ref for p in parts for ref in p[2]], *common)
        buffers = [
            pltpu.VMEM((size, buses), BF16),
            pltpu.VMEM((size, buses), BF16),
            pltpu.VMEM((size, buses), F32),
        ]
        if before:
            buffers = [pltpu.VMEM((size, buses), F32), *buffers, pltpu.SemaphoreType.DMA((2 + buses // BLOCK,))]
        return call(lambda *refs: kernel(at, insides, *refs), outs, n_in=len(ins), scratch=buffers, **more)(*ins)

    cut = rows - pieces[-1][1]
    done = ending(middle_kernel, 0, pieces[:-1], (), shape(cut, buses))
    final_state, plan2 = ending(
        end_kernel, cut, pieces[-1:], (done,), (shape(rows, buses), shape(hours, buses)), out_space=pl.ANY
    )
    return (final_state.reshape(start_state.shape), plan2[None])


def solution(mesh):
    in_specs = (
        P("region", "scen", None, None),
        P("region", "scen", None, None),
        P("region", "scen", None, None),
        P("region", None, None),
        P("region", None),
        P("region", None),
        P("region", None, None),
        P("region", None),
    )
    out_specs = (P("region", "scen", None, None), P("region", None, None))
    return jax.shard_map(inner, mesh=mesh, in_specs=in_specs, out_specs=out_specs, check_vma=False)
```

```python
import jax
import jax.numpy as jnp
from jax import lax
from jax.experimental import pallas as pl
from jax.experimental.pallas import tpu as pltpu
from jax.sharding import PartitionSpec as P


CHUNKS = (10, 6)
PARTS = ((4, 2, 4), (6,))
BLOCK = 256
step_rate = 0.3
tie_weight = 1.0
day_weight = 0.5


F32 = jnp.float32
BF16 = jnp.bfloat16


def dot(a, b):
    return lax.dot_general(a, b, (((1,), (0,)), ((), ())), preferred_element_type=F32)


def dot_t(a, b):
    return lax.dot_general(a, b, (((1,), (1,)), ((), ())), preferred_element_type=F32)


def high_low(x):
    high = x.astype(BF16)
    return high, (x - high.astype(F32)).astype(BF16)


def call(kernel, outs, *, n_in, scratch=(), out_space=pltpu.VMEM, flops=4 << 30):
    vmem = pl.BlockSpec(memory_space=pltpu.VMEM)
    out_spec = pl.BlockSpec(memory_space=out_space)
    return pl.pallas_call(
        kernel,
        out_shape=outs,
        in_specs=[vmem] * n_in,
        out_specs=jax.tree.map(lambda _: out_spec, outs),
        scratch_shapes=list(scratch),
        compiler_params=pltpu.CompilerParams(vmem_limit_bytes=16 << 20),
        cost_estimate=pl.CostEstimate(flops=flops, transcendentals=0, bytes_accessed=1 << 20),
    )


def over_scenarios(value, hours):
    rows, width = value.shape
    return jnp.sum(value.reshape(rows // hours, hours, width), axis=0)


def for_scenarios(value, rows):
    hours, width = value.shape
    return jnp.broadcast_to(value[None], (rows // hours, hours, width)).reshape(rows, width)


def over_blocks(width, one):
    for n in range(width // BLOCK):
        one(pl.ds(n * BLOCK, BLOCK))


def sum_kernel(state, out):
    hours = out.shape[0]

    def one(n, _):
        at = pl.ds(pl.multiple_of(n * BLOCK, BLOCK), BLOCK)
        out[:, at] = over_scenarios(state[:, at], hours)
        return 0

    lax.fori_loop(0, out.shape[1] // BLOCK, one, 0)


def select_kernel(index, out):
    rows = 128

    def one(n, _):
        start = pl.multiple_of(n * rows, rows)
        bus = lax.broadcasted_iota(jnp.int32, (rows, out.shape[1]), 0) + start
        out[pl.ds(start, rows), :] = jnp.where(bus == index[...], 1.0, 0.0).astype(BF16)
        return 0

    lax.fori_loop(0, out.shape[0] // rows, one, 0)


def split_into(pair, value, at):
    rows = value.shape[0]
    high, low = high_low(value)
    pair[:rows, at] = high
    pair[rows:, at] = low


def pick_kernel(start, sides, state, select, *refs):
    outs, pair = refs[:-1], refs[-1]
    rows, slots = outs[0].shape
    over_blocks(state.shape[1], lambda at: split_into(pair, state[start : start + rows, at], at))

    for side, out in zip(sides, outs):

        def one(at):
            both = dot(pair[...], select[:, pl.ds(side * slots + at.start, at.size)])
            out[:, at] = both[:rows] + both[rows:]

        over_blocks(slots, one)


def bounds_kernel(select, live, gen_bus, gen_cap, mask, upper):
    mask[...] = dot_t(jnp.broadcast_to(live[...], (8, live.shape[1])).astype(BF16), select[...])
    caps = jnp.broadcast_to(gen_cap[...], (8, gen_cap.shape[1]))
    high, rest = high_low(caps)
    middle, low = high_low(caps - high.astype(F32))
    del rest
    three = jnp.concatenate([high, middle, low], axis=0)
    rows = 128

    def one(n, _):
        start = pl.multiple_of(n * rows, rows)
        bus = lax.broadcasted_iota(jnp.int32, (rows, gen_bus.shape[1]), 0) + start
        chosen = jnp.where(bus == gen_bus[...], 1.0, 0.0).astype(BF16)
        parts = dot_t(three, chosen)
        upper[:, pl.ds(start, rows)] = parts[:8] + parts[8:16] + parts[16:]
        return 0

    lax.fori_loop(0, upper.shape[1] // rows, one, 0)


def theirs_into(pair, *ties):
    rows, at = pair.shape[0] // 2, 0
    for left, right in zip(ties[::2], ties[1::2]):
        size, slots = left.shape
        for start, side in ((0, left), (slots, right)):
            high, low = high_low(side[...])
            pair[at : at + size, start : start + slots] = high
            pair[rows + at : rows + at + size, start : start + slots] = low
        at += size


def theirs_at(pair, select, at):
    both = dot_t(pair[...], select[at, :])
    rows = both.shape[0] // 2
    return both[:rows] + both[rows:]


def stepped(now, slope, base, mask, lower, upper):
    slope = slope + base + (tie_weight * mask + day_weight) * now
    return jnp.minimum(jnp.maximum(now - step_rate * slope, lower), upper)


def first_kernel(start, *refs):
    state0, slope0, price, demand, matrix, select, left, right, mask, upper, plan = refs[:11]
    refs = refs[11:]
    out, dual_out, total, even, other, base, pair = refs
    rows, buses = out.shape
    hours = plan.shape[0]
    part = slice(start, start + rows)
    theirs_into(pair, left, right)

    def zero(at):
        now = state0[part, at]
        theirs = theirs_at(pair, select, at)
        middle = 0.5 * (now + theirs)
        dual = now - middle
        target = mask[:1, at] * (middle - dual)
        dual_out[:, at] = dual
        day_plan = for_scenarios(plan[:, at], rows)
        day_dual = now - day_plan
        constant = price[part, at] - tie_weight * mask[:1, at] * target + day_weight * (day_dual - day_plan)
        base[:, at] = constant
        new = stepped(now, slope0[part, at], constant, mask[:1, at], -demand[part, at], upper[:1, at])
        out[:, at] = new
        other[:, at] = new.astype(BF16)

    def one(at):
        new = stepped(out[:, at], dot(other[...], matrix[:, at]), base[:, at], mask[:1, at], -demand[part, at], upper[:1, at])
        out[:, at] = new
        even[:, at] = new.astype(BF16)

    def two(at):
        new = stepped(out[:, at], dot(even[...], matrix[:, at]), base[:, at], mask[:1, at], -demand[part, at], upper[:1, at])
        out[:, at] = new
        day_plan = for_scenarios(plan[:, at], rows)
        total[:, at] = over_scenarios(new + (state0[part, at] - day_plan), hours)

    over_blocks(buses, zero)
    over_blocks(buses, one)
    over_blocks(buses, two)


def prepare_kernel(start, inside, state0, state1, dual1, price, select, left, right, mask, plan1, base, pair):
    rows, buses = base.shape
    part = slice(start, start + rows)
    inner = slice(inside, inside + rows)
    theirs_into(pair, left, right)

    def zero(at):
        now = state1[inner, at]
        middle = 0.5 * (now + theirs_at(pair, select, at))
        dual = dual1[inner, at] + now - middle
        target = mask[:1, at] * (middle - dual)
        day_dual = state0[part, at] - for_scenarios(plan1[:, at], rows)
        base[:, at] = price[part, at] - tie_weight * mask[:1, at] * target + day_weight * (day_dual + now)

    over_blocks(buses, zero)


def early_kernel(state, matrix, slope, rounded):
    over_blocks(state.shape[1], lambda at: rounded.__setitem__((slice(None), at), state[:, at].astype(BF16)))

    def one(at):
        slope[:, at] = dot(rounded[...], matrix[:, at])

    over_blocks(state.shape[1], one)


def last_steps(start, insides, refs, written=None):
    pieces = [refs[3 * k : 3 * k + 3] for k in range(len(insides))]
    demand, matrix, mask, upper, plan, out, even, other, constants = refs[3 * len(insides) :]
    rows, buses = out.shape
    part = slice(start, start + rows)

    def zero(at):
        top = 0
        for inside, (state, slope, base) in zip(insides, pieces):
            size = base.shape[0]
            inner, here = slice(inside, inside + size), slice(top, top + size)
            lower = -demand[start + top : start + top + size, at]
            constant = base[:, at] - 2 * day_weight * for_scenarios(plan[:, at], size)
            constants[here, at] = constant
            new = stepped(state[inner, at], slope[inner, at], constant, mask[:1, at], lower, upper[:1, at])
            out[here, at] = new
            even[here, at] = new.astype(BF16)
            top += size

    def one(at):
        new = stepped(out[:, at], dot(even[...], matrix[:, at]), constants[:, at], mask[:1, at], -demand[part, at], upper[:1, at])
        out[:, at] = new
        other[:, at] = new.astype(BF16)

    def two(at):
        new = stepped(out[:, at], dot(other[...], matrix[:, at]), constants[:, at], mask[:1, at], -demand[part, at], upper[:1, at])
        out[:, at] = new
        if written is not None:
            written(at)

    over_blocks(buses, zero)
    over_blocks(buses, one)
    over_blocks(buses, two)


def middle_kernel(start, insides, *refs):
    last_steps(start, insides, refs)


def end_kernel(start, insides, *refs):
    done, state0, dual, price, select, left, right, plan1 = refs[:8]
    state, slope, demand, matrix, mask, upper, plan = refs[8:15]
    whole, plan_out, out, base, pair, even, other, constants, sems = refs[15:]
    rows = out.shape[0]
    copies = [
        pltpu.make_async_copy(plan, plan_out, sems.at[0]),
        pltpu.make_async_copy(done, whole.at[pl.ds(0, done.shape[0]), :], sems.at[1]),
    ]
    for copy in copies:
        copy.start()
    prepare_kernel(start, insides[0], state0, state, dual, price, select, left, right, mask, plan1, base, pair)

    def written(at):
        copy = pltpu.make_async_copy(
            out.at[:, at], whole.at[pl.ds(start, rows), at], sems.at[2 + at.start // BLOCK]
        )
        copy.start()
        copies.append(copy)

    ins = (state, slope, base, demand, matrix, mask, upper, plan)
    last_steps(start, insides, (*ins, out, even, other, constants), written)
    for copy in copies:
        copy.wait()


def flipped(size, bit):
    return [(i, i ^ bit) for i in range(size)]


def borders(size, first):
    pairs = [((i + first) % size, (i + first + 1) % size) for i in range(0, size, 2)]
    return [pair for a, b in pairs for pair in ((a, b), (b, a))]


def exchange(a, b):
    size = lax.axis_size("region")
    a = lax.ppermute(a, "region", borders(size, 0))
    b = lax.ppermute(b, "region", borders(size, 1))
    return a, b


def halves(total, core):
    size = lax.axis_size("scen")
    half = total.shape[1] // 2
    mine = jnp.where(core == 0, total[:, :half], total[:, half:])
    other = jnp.where(core == 0, total[:, half:], total[:, :half])
    return mine + lax.ppermute(other, "scen", flipped(size, 1))


def joined(part, core):
    back = lax.ppermute(part, "scen", flipped(lax.axis_size("scen"), 1))
    return jnp.where(
        core == 0, jnp.concatenate([part, back], axis=1), jnp.concatenate([back, part], axis=1)
    )


def from_flipped(value, bit):
    return lax.ppermute(value, "scen", flipped(lax.axis_size("scen"), bit))


def summed(total, core):
    part = halves(total, core)
    for bit in (16, 2):
        part = part + from_flipped(part, bit)
    a, b, c = [from_flipped(part, bit) for bit in (4, 8, 12)]
    return joined((part + a) + (b + c), core)


def inner(start_state, price, demand, sens, gen_bus, gen_cap, tie_index, tie_len):
    scens, hours, buses = start_state.shape[1:]
    slots = tie_index.shape[2]
    rows = scens * hours
    total_scen = scens * lax.axis_size("scen")
    state0 = start_state.reshape(rows, buses)
    prices = price.reshape(rows, buses)
    demands = demand.reshape(rows, buses)
    matrix = sens[0]
    core = lax.axis_index("scen") % 2
    odd = lax.axis_index("region") % 2

    def by_border(pair):
        return jnp.where(odd == 0, jnp.concatenate([pair[1], pair[0]]), jnp.concatenate([pair[0], pair[1]]))[None]

    index = by_border(tie_index[0])
    live = (jnp.arange(slots, dtype=jnp.int32)[None, :] < tie_len[0][:, None]).astype(F32)
    live = by_border(live)

    def shape(*dims, dtype=F32):
        return jax.ShapeDtypeStruct(dims, dtype)

    def pick(at, state, size, sides=(0, 1)):
        return call(
            lambda *refs: pick_kernel(at, sides, *refs),
            (shape(size, slots),) * len(sides),
            n_in=2,
            scratch=[pltpu.VMEM((2 * size, buses), BF16)],
        )(state, select)

    total0 = call(sum_kernel, shape(hours, buses), n_in=1, flops=1 << 20)(state0)
    select = call(select_kernel, shape(buses, 2 * slots, dtype=BF16), n_in=1, flops=1 << 20)(index)
    starts = [sum(CHUNKS[:c]) * hours for c in range(len(CHUNKS))]
    sizes = [c * hours for c in CHUNKS]
    theirs = []
    for c, (at, size) in enumerate(zip(starts, sizes)):
        if c == 0:
            picked = pick(at, state0, size, (0,)) + pick(at, state0, size, (1,))
        else:
            picked = pick(at, state0, size)
        theirs.append(exchange(*picked))

    def early(state):
        return call(early_kernel, shape(*state.shape), n_in=2, scratch=[pltpu.VMEM(state.shape, BF16)])(state, matrix)

    slope0 = early(state0)
    mask, upper = call(bounds_kernel, (shape(8, buses), shape(8, buses)), n_in=4)(select, live, gen_bus, gen_cap)
    plan1 = summed(total0, core) / total_scen

    firsts = []
    theirs1 = []
    for c, (at, size) in enumerate(zip(starts, sizes)):
        wide = shape(size, buses)
        first = call(
            lambda *refs, at=at: first_kernel(at, *refs),
            (wide, wide, shape(hours, buses)),
            n_in=11,
            scratch=[
                pltpu.VMEM((size, buses), BF16),
                pltpu.VMEM((size, buses), BF16),
                pltpu.VMEM((size, buses), F32),
                pltpu.VMEM((2 * size, buses), BF16),
            ],
        )(state0, slope0, prices, demands, matrix, select, *theirs[c], mask, upper, plan1)
        firsts.append(first)
        inside = 0
        for k, part in enumerate(PARTS[c]):
            picked = pick(inside, first[0], part * hours)
            theirs1.append((c, k, inside, part * hours, exchange(*picked)))
            inside += part * hours
    total1 = sum(f[2] for f in firsts[1:]) + firsts[0][2]
    slopes = [early(first[0]) for first in firsts]
    pieces = []
    for c, k, inside, size, ties in theirs1[:-1]:
        base = call(
            lambda *refs, at=starts[c] + inside, inside=inside: prepare_kernel(at, inside, *refs),
            shape(size, buses),
            n_in=9,
            scratch=[pltpu.VMEM((2 * size, buses), BF16)],
        )(state0, firsts[c][0], firsts[c][1], prices, select, *ties, mask, plan1)
        pieces.append((inside, size, (firsts[c][0], slopes[c], base)))
    plan2 = summed(total1, core) / total_scen
    common = (demands, matrix, mask, upper, plan2)

    def ending(kernel, at, size, insides, ins, outs, more=(), **kwargs):
        buffers = [
            *more,
            pltpu.VMEM((size, buses), BF16),
            pltpu.VMEM((size, buses), BF16),
            pltpu.VMEM((size, buses), F32),
        ]
        if more:
            buffers.append(pltpu.SemaphoreType.DMA((2 + buses // BLOCK,)))
        return call(lambda *refs: kernel(at, insides, *refs), outs, n_in=len(ins), scratch=buffers, **kwargs)(*ins)

    c, _, inside, size, ties = theirs1[-1]
    cut = rows - size
    done = ending(
        middle_kernel,
        0,
        cut,
        tuple(p[0] for p in pieces),
        (*[ref for p in pieces for ref in p[2]], *common),
        shape(cut, buses),
    )
    final_state, plan2 = ending(
        end_kernel,
        cut,
        size,
        (inside,),
        (done, state0, firsts[c][1], prices, select, *ties, plan1, firsts[c][0], slopes[c], *common),
        (shape(rows, buses), shape(hours, buses)),
        more=(
            pltpu.VMEM((size, buses), F32),
            pltpu.VMEM((size, buses), F32),
            pltpu.VMEM((2 * size, buses), BF16),
        ),
        out_space=pl.ANY,
    )
    return (final_state.reshape(start_state.shape), plan2[None])


def solution(mesh):
    in_specs = (
        P("region", "scen", None, None),
        P("region", "scen", None, None),
        P("region", "scen", None, None),
        P("region", None, None),
        P("region", None),
        P("region", None),
        P("region", None, None),
        P("region", None),
    )
    out_specs = (P("region", "scen", None, None), P("region", None, None))
    return jax.shard_map(inner, mesh=mesh, in_specs=in_specs, out_specs=out_specs, check_vma=False)
```
